32 devices in a mesh: dp: 16 (over z, y, core), tensor: 2 (over x).
Axes of the slice: x: 2, y: 2, z: 4, core: 2. Of those that a mesh axis runs over, the one named last changes fastest.
Arguments:
- expert_act: bfloat16 [16384, 2880], P(('dp', 'tensor')), may hold values from -6 to 6
- grad_out: bfloat16 [32768, 1440], P(('dp', 'tensor')), may hold values from -6 to 6
- slot_token: int32 [16384], P(('dp', 'tensor')), may hold values from 0 to 1023, as said below
- slot_prob: float32 [16384], P(('dp', 'tensor')), may hold values from 0.2 to 1
- live_count: int32 [32], P(('dp', 'tensor')), may hold values from 128 to 512, as said below
Outputs:
- weight_grad: float32 [2880, 1440], P('dp', 'tensor')
The draws below stay inside these ranges and needn't reach their ends.
Inputs may be any that keep to these rules, and one draw needn't show every extreme that they name: `slot_token`: each device's 512 entries are distinct token indices of that device. `live_count`: each entry is 512 // j for some j of 1 to 4.
All inputs are finite; a program needn't handle non-finite values.
Results may differ from the reference program's by a relative error of at most 0.0029.
Values may be sent and summed in bfloat16 or wider, within the bound.
No kernel may reach another device: no remote copies, remote signals or barrier semaphores. Data moves between devices by JAX's collectives and lax.ppermute only.
A program may use at most 128 MiB of HBM per device.

```python
import math
import jax
import jax.numpy as jnp
from jax import lax

D = 1440
FF = 2880
CAP = 512
TOK_DEV = 1024
SLOTS = 16384
TOKENS = 32768


def draw_slot_token(key, part):
    device_total = SLOTS // CAP
    device_keys = jax.random.split(jax.random.fold_in(key, 11), device_total)

    def shuffled(seed_key):
        return jax.random.permutation(seed_key, TOK_DEV)[:CAP].astype(jnp.int32)
    return jax.vmap(shuffled)(device_keys).reshape(-1).astype(jnp.int32)


def draw_live_count(key, part):
    device_total = SLOTS // CAP
    first_key = jax.random.fold_in(key, 21)
    second_key = jax.random.fold_in(key, 22)
    divisor = jax.random.randint(first_key, (device_total,), 1, 5)
    counted = (CAP // divisor).astype(jnp.int32)
    fullest = jax.random.randint(second_key, (), 0, device_total)
    return counted.at[fullest].set(CAP).astype(jnp.int32)


def block_levels(key, shape, shards, low, high):
    factor_of = 1.0
    for dim, blocks in shards:
        steps = jax.random.uniform(jax.random.fold_in(jax.random.fold_in(key, 6), dim), (blocks,), jnp.float32, low / len(shards), high / len(shards))
        factor_of = factor_of * jnp.repeat(jnp.exp(steps), shape[dim] // blocks).reshape((-1,) + (1,) * (len(shape) - 1 - dim))
    return factor_of


def normal_values(stream_key, dims, width, reach, pieces=(), kind=jnp.bfloat16):
    entries = jax.random.normal(stream_key, dims, jnp.float32) * width
    if len(pieces) > 0:
        entries = block_levels(stream_key, dims, pieces, -0.22, 0.18) * entries
    return jnp.clip(entries, min=-reach, max=reach).astype(kind)


def setup_inputs(seed: int = 0) -> dict:
    splits = jax.random.split(jax.random.key(seed), 6)
    expert_act = normal_values(splits[0], (SLOTS, FF), 1.0, 6.0, ((0, 32),))
    grad_out = normal_values(splits[1], (TOKENS, D), 1.0, 6.0, ((0, 32),))
    slot_token = draw_slot_token(jax.random.fold_in(splits[5], 71), 0)
    slot_prob = jnp.clip(jnp.exp(math.log(1.0) - 1.609438 * jax.random.uniform(splits[3], (SLOTS,), jnp.float32) ** block_levels(splits[3], (SLOTS,), ((0, 32),), -0.2, 0.2)), 0.2, 1.0)
    live_count = draw_live_count(jax.random.fold_in(splits[5], 71), 0)
    return dict(expert_act=expert_act, grad_out=grad_out, slot_token=slot_token, slot_prob=slot_prob, live_count=live_count)


def reference(expert_act, grad_out, slot_token, slot_prob, live_count):
    slot_total = expert_act.shape[0]
    position = jnp.arange(slot_total, dtype=jnp.int32)
    owner_dev = (position // CAP).astype(jnp.int32)
    token_rows = (slot_token + owner_dev * TOK_DEV).astype(jnp.int32)
    live_mask = position % CAP < live_count[owner_dev]
    weighting = jnp.where(live_mask, slot_prob, jnp.zeros_like(slot_prob))
    picked = grad_out[token_rows].astype(jnp.float32)
    weighted = (picked * weighting[:, None]).astype(jnp.bfloat16)
    gradient = lax.dot_general(expert_act, weighted, (((0,), (0,)), ((), ())), preferred_element_type=jnp.float32)
    return gradient * (1.0 / math.sqrt(slot_total))
```

```python
import functools
import itertools
import itertools
import itertools
import itertools
import itertools
import itertools
import itertools
import math

import jax
import jax.numpy as jnp
from jax import lax
from jax.experimental import pallas as pl
from jax.experimental.pallas import tpu as pltpu
from jax.sharding import PartitionSpec as P


CHIP_BITS = "YNF"
ROUTES = (('YXNF', 10), ('XNFY', 8), ('NXYF', 5))
SPLIT = frozenset(((0, 0), (0, 1), (0, 2), (1, 0), (1, 1), (1, 2), (2, 0), (2, 1), (2, 2)))
ORDER = ((1, 0, 1), (1, 0, 0), (0, 0, 1), (2, 0, 1), (1, 1, 1), (2, 0, 0), (1, 1, 0), (0, 0, 0), (2, 1, 1), (0, 1, 1), (2, 1, 0), (0, 1, 0), (1, 2, 1), (1, 2, 0), (2, 2, 1), (2, 2, 0), (0, 2, 1), (0, 2, 0), (2, 3, None), (0, 3, None), (1, 3, None))
TILE = 256
GRANT = 24 * 1024 * 1024
WEIGH_GRANT = 50 * 1024 * 1024


def contract(left, right):
    return lax.dot_general(
        left, right, (((0,), (0,)), ((), ())), preferred_element_type=jnp.float32
    )


def plain(expert_act, grad_out, slot_token, slot_prob, live_count):
    slot_count = expert_act.shape[0]
    devices = lax.axis_size("dp") * lax.axis_size("tensor")
    scaling = 1.0 / math.sqrt(slot_count * devices)
    position = jnp.arange(slot_count, dtype=jnp.int32)
    live_mask = position < live_count[0]
    weighting = jnp.where(live_mask, slot_prob, jnp.zeros_like(slot_prob))
    picked = jnp.take(grad_out, slot_token, axis=0).astype(jnp.float32)
    weighted = (picked * weighting[:, None]).astype(jnp.bfloat16)
    both_acts = lax.all_gather(expert_act, "tensor", axis=0, tiled=True)
    both_grads = lax.all_to_all(weighted, "tensor", split_axis=1, concat_axis=0, tiled=True)
    gradient = lax.psum_scatter(
        contract(both_acts, both_grads), "dp", scatter_dimension=0, tiled=True
    )
    return gradient * scaling


def weigh_kernel(grad, token, prob, live, out1, out0, rows, onehot, sems):
    tokens, slots = onehot.shape
    count, tile, _ = rows.shape
    steps, wide = count // 2, out1.shape[0]
    half = steps * tile
    x = lax.axis_index("tensor")
    copies = []
    for i in range(count):
        side, t = 1 - i // steps, i % steps
        start = pl.multiple_of(half * (x ^ side) + t * tile, 8)
        copy = pltpu.make_async_copy(grad.at[pl.ds(start, tile), :], rows.at[i], sems.at[i])
        copy.start()
        copies.append(copy)
    wanted = jnp.broadcast_to(token[...], (128, slots))
    for t in range(0, tokens, 128):
        here = lax.broadcasted_iota(jnp.int32, (128, slots), 0) + t
        onehot[t : t + 128, :] = jnp.where(here == wanted, 1.0, 0.0).astype(jnp.bfloat16)
    position = lax.broadcasted_iota(jnp.int32, (1, slots), 1)
    weight = jnp.where(position < live[0], prob[...], 0.0)
    for i in range(count):
        out, t = (out1, out0)[i // steps], i % steps
        copies[i].wait()
        picked = jnp.dot(rows[i], onehot[...], preferred_element_type=jnp.float32)
        out[t * tile : (t + 1) * tile, :] = (picked * weight).astype(jnp.bfloat16)
    if wide > half:
        for out in (out1, out0):
            out[half:, :] = jnp.zeros((wide - half, slots), jnp.bfloat16)


def weigh(grad, token, prob, live):
    width, tokens = grad.shape
    slots = token.shape[1]
    half = width // 2
    wide = -(-half // TILE) * TILE
    tile = next(t for t in range(min(half, 360), 0, -1) if half % t == 0 and t % 8 == 0)
    vmem = pl.BlockSpec(memory_space=pltpu.VMEM)
    hbm = pl.BlockSpec(memory_space=pltpu.HBM)
    line = pl.BlockSpec((1, slots), lambda i: (0, 0))
    return pl.pallas_call(
        weigh_kernel,
        grid=(1,),
        out_shape=[jax.ShapeDtypeStruct((wide, slots), jnp.bfloat16)] * 2,
        in_specs=[hbm, line, line, pl.BlockSpec(memory_space=pltpu.SMEM)],
        out_specs=[vmem] * 2,
        scratch_shapes=[
            pltpu.VMEM((width // tile, tile, tokens), jnp.bfloat16),
            pltpu.VMEM((tokens, slots), jnp.bfloat16),
            pltpu.SemaphoreType.DMA((width // tile,)),
        ],
        cost_estimate=pl.CostEstimate(
            flops=2 * width * tokens * slots, bytes_accessed=2 * width * tokens, transcendentals=0
        ),
        compiler_params=pltpu.CompilerParams(vmem_limit_bytes=WEIGH_GRANT),
        name="weigh",
    )(grad, token, prob, live)


def product_kernel(jobs, block, slab, n_out, acts_own, acts_other, *rest):
    sides = sorted(jobs, reverse=True)
    w = {a: rest[2 * i : 2 * i + 2] for i, a in enumerate(sides)}
    rest = rest[2 * len(sides) :]
    outs, (left,) = rest[:n_out], rest[n_out:]
    chip = lax.axis_index("dp") // 2
    core = lax.axis_index("dp") % 2
    wide, slots = w[sides[0]][0].shape
    base = 0
    for a in sides:
        at = base
        for q, row, n, _, _ in jobs[a]:
            start = pl.multiple_of(block * (chip ^ q) + (block - slab) * core + row, 8)
            left[at : at + n, :slots] = acts_own[pl.ds(start, n), :]
            left[at : at + n, slots:] = acts_other[pl.ds(start, n), :]
            at += n
        rows = at - base

        @pl.loop(0, wide, step=TILE)
        def _(t):
            t = pl.multiple_of(t, TILE)
            total = None
            for s, right in enumerate(w[a]):
                term = lax.dot_general(
                    left[base : base + rows, s * slots : (s + 1) * slots],
                    right[pl.ds(t, TILE), :],
                    (((1,), (1,)), ((), ())),
                    preferred_element_type=jnp.float32,
                )
                total = term if total is None else total + term
            at = 0
            for _, _, n, out, index in jobs[a]:
                outs[out][index + (slice(None), pl.ds(t, TILE))] = total[at : at + n].astype(
                    outs[out].dtype
                )
                at += n

        base += rows


def product(jobs, shapes, block, slab, acts_own, acts_other, w):
    rows = sum(job[2] for a in jobs for job in jobs[a])
    wide, slots = w[0][0].shape
    weights = [value for a in sorted(jobs, reverse=True) for value in w[a]]
    vmem = pl.BlockSpec(memory_space=pltpu.VMEM)
    return pl.pallas_call(
        functools.partial(product_kernel, jobs, block, slab, len(shapes)),
        out_shape=[jax.ShapeDtypeStruct(s, t) for s, t in shapes],
        in_specs=[vmem] * (2 + len(weights)),
        out_specs=[vmem] * len(shapes),
        scratch_shapes=[pltpu.VMEM((rows, 2 * slots), jnp.bfloat16)],
        cost_estimate=pl.CostEstimate(
            flops=4 * rows * wide * slots,
            bytes_accessed=4 * (rows + 2 * wide) * slots,
            transcendentals=0,
        ),
        compiler_params=pltpu.CompilerParams(vmem_limit_bytes=GRANT),
    )(acts_own, acts_other, *weights)


def finish_kernel(groups, skip, scaling, *refs):
    ins, out = refs[:-1], refs[-1]
    rows, half = out.shape
    core = lax.axis_index("dp") % 2
    parts, at = [], 0
    for count in groups:
        total = None
        for ref in ins[at : at + count]:
            value = ref[(0,) * (len(ref.shape) - 2)].astype(jnp.float32)
            total = value if total is None else total + value
        parts.append(total[:, :half])
        at += count
    whole = jnp.concatenate(parts, axis=0)
    picked = jnp.where(core == 0, whole[:rows], whole[skip : skip + rows])
    out[...] = picked * scaling


def finish(groups, rows, half, skip, scaling, terms):
    vmem = pl.BlockSpec(memory_space=pltpu.VMEM)
    return pl.pallas_call(
        functools.partial(finish_kernel, groups, skip, scaling),
        out_shape=jax.ShapeDtypeStruct((rows, half), jnp.float32),
        in_specs=[vmem] * len(terms),
        out_specs=vmem,
        compiler_params=pltpu.CompilerParams(vmem_limit_bytes=GRANT),
        name="finish",
    )(*terms)


def shares(slab):
    groups, total = slab // 8, sum(share for _, share in ROUTES)
    marks, seen = [0], 0
    for _, share in ROUTES:
        seen += share
        marks.append(8 * round(groups * seen / total))
    return marks


def plan_of(r, i):
    return f"part_{r}_{i}" if i < 2 else "part_rest"


def staged(expert_act, grad_out, slot_token, slot_prob, live_count):
    dp, tp = lax.axis_size("dp"), lax.axis_size("tensor")
    slot_count, wide = expert_act.shape
    half = grad_out.shape[1] // 2
    lanes = -(-half // TILE) * TILE
    scaling = 1.0 / math.sqrt(slot_count * dp * tp)
    block = wide // (dp // 2)
    rows = block // 2
    slab = -(-rows // 8) * 8
    f32, bf16 = jnp.float32, jnp.bfloat16
    depth = len(ROUTES[0][0])

    def send(value, step):
        if step == "X":
            return lax.ppermute(value, "tensor", [(0, 1), (1, 0)])
        flip = 1 if step == "core" else 2 << CHIP_BITS.index(step)
        return lax.ppermute(value, "dp", [(i, i ^ flip) for i in range(dp)])

    def owner(route, bits):
        a, q = 0, 0
        for step, bit in zip(route, bits):
            if step == "X":
                a = bit
            else:
                q |= bit << CHIP_BITS.index(step)
        return a, q

    acts = expert_act.T
    other_acts = send(acts, "core")
    routed = grad_out.T, slot_token[None], slot_prob[None], live_count
    w1, w0 = weigh(*routed)
    other_w1 = send(w1, "core")
    other_w0 = send(w0, "core")
    w = (w0, other_w0), (w1, other_w1)

    marks = shares(slab)
    plans = {}

    def want(plan, key, dtype, route, head, row, n):
        jobs, shapes, keys = plans.setdefault(plan, ({}, [], []))
        free = depth - len(head)
        for index in itertools.product(range(2), repeat=free):
            a, q = owner(route, head + index)
            jobs.setdefault(a, []).append((q, row, n, len(shapes), index))
        shapes.append(((2,) * free + (n, lanes), dtype))
        keys.append(key)

    for r, (route, _) in enumerate(ROUTES):
        row, n = marks[r], marks[r + 1] - marks[r]
        for i in range(depth):
            plan, dtype = plan_of(r, i), f32 if i else bf16
            head = (0,) * i + (1,)
            if (r, i) in SPLIT:
                want(plan, (r, i, 1), dtype, route, head + (1,), row, n)
                want(plan, (r, i, 0), dtype, route, head + (0,), row, n)
            else:
                want(plan, (r, i, None), dtype, route, head, row, n)
        want(plan_of(r, depth), (r, depth), f32, route, (0,) * depth, row, n)

    part = {}
    for (jobs, shapes, keys) in plans.values():
        values = product(jobs, shapes, block, slab, acts, other_acts, w)
        part.update(zip(keys, values))

    got = {}

    def received(r, i, bits):
        if (r, i) in SPLIT:
            return got[r, i, bits[0]][tuple(bits[1:])]
        return got[r, i, None][tuple(bits)]

    def emit(r, i, which):
        value = part[r, i, which]
        if i > 0:
            extra = () if which is None else (which,)
            for j in range(i):
                value = value + received(r, j, (0,) * (i - j - 1) + (1,) + extra).astype(f32)
            value = value.astype(bf16)
        got[r, i, which] = send(value, ROUTES[r][0][i])

    for r, i, which in ORDER:
        emit(r, i, which)

    terms, groups = [], []
    for r in range(len(ROUTES)):
        terms.append(part[r, depth])
        for i in range(depth):
            terms.append(got[r, i, 0 if (r, i) in SPLIT else None])
        groups.append(depth + 1)
    return finish(groups, rows, half, slab - rows, scaling, terms)


def solution(mesh):
    dp, tp = mesh.shape["dp"], mesh.shape["tensor"]

    def shards(expert_act, grad_out, slot_token, slot_prob, live_count):
        wide, width = expert_act.shape[1], grad_out.shape[1]
        fits = (
            tp == 2
            and dp == 2 << len(CHIP_BITS)
            and wide % (4 * dp) == 0
            and width % 16 == 0
            and expert_act.shape[0] % 128 == 0
            and grad_out.shape[0] % 128 == 0
        )
        form = staged if fits else plain
        return form(expert_act, grad_out, slot_token, slot_prob, live_count)

    return jax.shard_map(
        shards,
        mesh=mesh,
        in_specs=(
            P(("dp", "tensor"), None),
            P(("dp", "tensor"), None),
            P(("dp", "tensor")),
            P(("dp", "tensor")),
            P(("dp", "tensor")),
        ),
        out_specs=P("dp", "tensor"),
        check_vma=False,
    )
```
